32 devices in a mesh: dp: 16 (over z, y, core), rep: 2 (over x).
Axes of the slice: x: 2, y: 2, z: 4, core: 2. Of those that a mesh axis runs over, the one named last changes fastest.
Arguments:
- gate_pre: bfloat16 [2, 2048, 5632], P(None, 'dp', 'rep'), may hold values from -8 to 8
- up_pre: bfloat16 [2, 2048, 5632], P(None, 'dp', 'rep'), may hold values from -6 to 6
- out_grad: bfloat16 [2, 2048, 1024], P(None, 'dp'), may hold values from -6 to 6
- master: float32 [1024, 5632], P('dp', 'rep'), may hold values from -0.078125 to 0.078125
- moment_one: float32 [1024, 5632], P('dp', 'rep'), may hold values from -0.02 to 0.02
- moment_two: float32 [1024, 5632], P('dp', 'rep'), may hold values from 1e-06 to 1e-05
Outputs:
- layer_out: bfloat16 [2, 2048, 1024], P(None, 'dp', 'rep')
- gate_grad: bfloat16 [2, 2048, 5632], P(None, 'dp', 'rep')
- up_grad: bfloat16 [2, 2048, 5632], P(None, 'dp', 'rep')
- master_new: float32 [1024, 5632], P('dp', 'rep')
- moment_one_new: float32 [1024, 5632], P('dp', 'rep')
- moment_two_new: float32 [1024, 5632], P('dp', 'rep')
The draws below stay inside these ranges and needn't reach their ends.
All inputs are finite; a program needn't handle non-finite values.
Results may differ from the reference program's by a relative error of at most 0.0048.
The reference program's roundings to bfloat16 on the way (of `weight_bf` and `hidden`) count: a program that leaves them out, or rounds other values in their place, can miss the bound.
Values may be sent and summed in bfloat16 or wider, within the bound.
No kernel may reach another device: no remote copies, remote signals or barrier semaphores. Data moves between devices by JAX's collectives and lax.ppermute only.
A program may use at most 128 MiB of HBM per device.

```python
import math
import jax
import jax.numpy as jnp
from jax import lax

D = 1024
FF = 5632
MB = 2
TOKENS = 2048


def strengthened(values, stream_key, source, target, shards_of, factor):
    def block_of(axis_at):
        return (jnp.arange(values.shape[axis_at]) // (values.shape[axis_at] // shards_of)).reshape((-1,) + (1,) * (values.ndim - 1 - axis_at))

    one_side = jax.random.permutation(stream_key, shards_of)[block_of(target)]
    far = (block_of(target) + shards_of // 2) % shards_of
    return jnp.where((block_of(source) == one_side) | (block_of(source) == far), factor * values, values)


def shard_levels(rng, shape, pieces, smallest, top_value):
    level, own = 1.0, jax.random.fold_in(rng, 6)
    for axis_at, blocks in pieces:
        draws = jnp.exp(jax.random.uniform(jax.random.fold_in(own, axis_at), (blocks,), jnp.float32, smallest / len(pieces), top_value / len(pieces)))
        level = level * jnp.repeat(draws, shape[axis_at] // blocks).reshape([-1 if axis == axis_at else 1 for axis in range(len(shape))])
    return level


def centred(rng, extent, width, most, pieces=(), held_as=jnp.bfloat16):
    array = jax.random.normal(rng, extent, jnp.float32) * width
    if len(pieces) > 0:
        array = shard_levels(rng, extent, pieces, -0.22, 0.18) * array
    return jnp.clip(array, min=-most, max=most).astype(held_as)


def heavy_noise(key, shape, scale, reach, pieces, heavy, dtype=jnp.bfloat16):
    drawn = scale * jax.random.normal(key, shape, jnp.float32)
    if pieces:
        drawn = drawn * shard_levels(key, shape, pieces, -0.22, 0.18)
    return jnp.clip(strengthened(drawn, jax.random.fold_in(key, 3), *heavy), -reach, reach).astype(dtype)


def setup_inputs(seed: int = 0) -> dict:
    splits = jax.random.split(jax.random.key(seed), 7)
    gate_pre = centred(splits[0], (MB, TOKENS, FF), 1.5, 8.0, ((1, 16), (2, 2)))
    up_pre = centred(splits[1], (MB, TOKENS, FF), 1.0, 6.0, ((1, 16), (2, 2)))
    out_grad = heavy_noise(splits[2], (MB, TOKENS, D), 1.0, 6.0, ((1, 16),), (1, 2, 16, 2.0))
    master = centred(splits[3], (D, FF), FF ** -0.5, 0.078125, ((0, 16), (1, 2)), jnp.float32)
    moment_one = centred(splits[4], (D, FF), 0.003, 0.02, ((0, 16), (1, 2)), jnp.float32)
    moment_two = jnp.clip(jnp.exp(math.log(9.999999747378752e-06) - 2.3025851 * jax.random.uniform(splits[5], (D, FF), jnp.float32) ** shard_levels(splits[5], (D, FF), ((0, 16), (1, 2)), -0.2, 0.2)), 9.999999974752427e-07, 9.999999747378752e-06)
    return {"gate_pre": gate_pre, "up_pre": up_pre, "out_grad": out_grad, "master": master, "moment_one": moment_one, "moment_two": moment_two}


first_power = 2.6561398887587544e-05
second_power = 0.005920529220333997

def reference(gate_pre, up_pre, out_grad, master, moment_one, moment_two):
    weight_bf = master.astype(jnp.bfloat16)
    outs_list = []
    gate_list = []
    up_list = []
    grad_sum = jnp.zeros(master.shape, jnp.float32)
    for index in range(MB):
        gate = gate_pre[index].astype(jnp.float32)
        up_val = up_pre[index].astype(jnp.float32)
        sig = jax.nn.sigmoid(gate)
        hidden = (gate * sig * up_val).astype(jnp.bfloat16)
        result = lax.dot_general(hidden, weight_bf, (((1,), (1,)), ((), ())), preferred_element_type=jnp.float32)
        outs_list.append(result.astype(jnp.bfloat16))
        hid_grad = jnp.dot(out_grad[index], weight_bf, preferred_element_type=jnp.float32)
        gate_list.append((hid_grad * up_val * sig * (1.0 + gate * (1.0 - sig))).astype(jnp.bfloat16))
        up_list.append((hid_grad * gate * sig).astype(jnp.bfloat16))
        grad_sum = grad_sum + lax.dot_general(out_grad[index], hidden, (((0,), (0,)), ((), ())), preferred_element_type=jnp.float32)
    main_grad = grad_sum / jnp.float32(MB * TOKENS)
    first = 0.9 * moment_one + 0.1 * main_grad
    second = 0.95 * moment_two + 0.05 * main_grad * main_grad
    update = first / (1.0 - first_power) / (jnp.sqrt(second / (1.0 - second_power)) + 1e-08)
    master_new = master - 0.003 * (update + 0.1 * master)
    return (jnp.stack(outs_list), jnp.stack(gate_list), jnp.stack(up_list), master_new, first, second)
```

```python
import functools
import jax
import jax.numpy as jnp
from jax import lax
from jax.experimental import pallas as pl
from jax.experimental.pallas import tpu as pltpu
from jax.sharding import PartitionSpec as P


first_power = 2.6561398887587544e-05
second_power = 0.005920529220333997


VMEM = pl.BlockSpec(memory_space=pltpu.VMEM)
SMEM = pl.BlockSpec(memory_space=pltpu.SMEM)
TILE = 256


def adamw(main_grad, master, moment_one, moment_two):
    first = 0.9 * moment_one + 0.1 * main_grad
    second = 0.95 * moment_two + 0.05 * main_grad * main_grad
    update = first / (1.0 - first_power) / (jnp.sqrt(second / (1.0 - second_power)) + 1e-08)
    return master - 0.003 * (update + 0.1 * master), first, second


def gated(gate, up_val):
    gate = gate.astype(jnp.float32)
    return (gate * jax.nn.sigmoid(gate) * up_val.astype(jnp.float32)).astype(jnp.bfloat16)


def plain(gate_pre, up_pre, out_grad, master, moment_one, moment_two):
    micro, rows, width = gate_pre.shape
    total = micro * rows * lax.axis_size("dp")
    weights = lax.all_gather(master.astype(jnp.bfloat16), "dp", axis=0, tiled=True)
    hidden = gated(gate_pre, up_pre).reshape(-1, width)
    cotangent = out_grad.reshape(-1, out_grad.shape[2])
    grads = lax.dot_general(
        cotangent, hidden, (((0,), (0,)), ((), ())), preferred_element_type=jnp.float32
    )
    part = lax.dot_general(
        hidden, weights, (((1,), (1,)), ((), ())), preferred_element_type=jnp.float32
    )
    hid_grad = jnp.dot(cotangent, weights, preferred_element_type=jnp.float32)
    grads = lax.psum_scatter(grads, "dp", scatter_dimension=0, tiled=True)
    out = lax.psum_scatter(part, "rep", scatter_dimension=1, tiled=True).astype(jnp.bfloat16)
    gate = gate_pre.reshape(-1, width).astype(jnp.float32)
    up_val = up_pre.reshape(-1, width).astype(jnp.float32)
    sig = jax.nn.sigmoid(gate)
    gate_grad = (hid_grad * up_val * sig * (1.0 + gate * (1.0 - sig))).astype(jnp.bfloat16)
    up_grad = (hid_grad * gate * sig).astype(jnp.bfloat16)
    master_new, first, second = adamw(
        grads / jnp.float32(total), master, moment_one, moment_two
    )
    return (
        out.reshape(micro, rows, -1),
        gate_grad.reshape(gate_pre.shape),
        up_grad.reshape(gate_pre.shape),
        master_new,
        first,
        second,
    )


def select_kernel(zs, rows, me_ref, og_ref, *refs):
    outs, turned = refs[:4], refs[4]
    turned[...] = og_ref[...].T
    me = me_ref[0]
    for m in range(4):
        for s in range(zs):
            start = pl.multiple_of(((me ^ (4 * s)) ^ m) * rows, rows)
            outs[m][s * rows : (s + 1) * rows, :] = turned[pl.ds(start, rows), :]


def turn_kernel(*refs):
    count = len(refs) // 2
    for source, target in zip(refs[:count], refs[count:]):
        target[...] = source[...].T


def each_tile(width, body):
    for start in range(0, width, TILE):
        body(slice(start, start + TILE))


def grads_kernel(zs, rows, *refs):
    lefts, rights, outs = refs[:4], refs[4:8], refs[8 : 8 + zs]

    def body(at):
        total = None
        for left, right in zip(lefts, rights):
            term = jnp.dot(left[...], right[:, at], preferred_element_type=jnp.float32)
            total = term if total is None else total + term
        for s in range(zs):
            outs[s][:, at] = total[s * rows : (s + 1) * rows, :].astype(outs[s].dtype)

    each_tile(rights[0].shape[1], body)


def stacked(chunks, at):
    return jnp.concatenate([chunk[:, at] for chunk in chunks], axis=0)


def out_rows(zs, me_ref, rep_ref, turned, chunks, keep, send, total):
    base, value = 0, None
    for piece in turned:
        at = slice(base, base + piece.shape[0])
        term = jnp.dot(stacked(chunks, at), piece[...], preferred_element_type=jnp.float32)
        value = term if value is None else value + term
        base = at.stop
    total[...] = value
    half = keep.shape[0]
    flip = ((me_ref[0] // (2 * zs)) ^ rep_ref[0]) & 1
    keep[...] = total[pl.ds(pl.multiple_of(flip * half, half), half), :]
    send[...] = total[pl.ds(pl.multiple_of((1 - flip) * half, half), half), :]


def near_kernel(zs, me_ref, rep_ref, *refs):
    turned, (one, two), chunks = refs[:2], refs[2:4], refs[4 : 4 + 2 * zs]
    keep, send, early, left, total = refs[4 + 2 * zs :]
    out_rows(zs, me_ref, rep_ref, turned, chunks, keep, send, total)
    width = one.shape[0]
    left[:, :width] = one[...].T
    left[:, width:] = two[...].T
    order = chunks[0::2] + chunks[1::2]

    def body(at):
        early[:, at] = jnp.dot(
            left[...], stacked(order, at), preferred_element_type=jnp.float32
        )

    each_tile(early.shape[1], body)


def far_kernel(zs, me_ref, rep_ref, *refs):
    turned, chunks = refs[:2], refs[2 : 2 + 2 * zs]
    keep, send, total = refs[2 + 2 * zs :]
    out_rows(zs, me_ref, rep_ref, turned, chunks, keep, send, total)


def back_kernel(zs, *refs):
    (one, two, gate_ref, up_ref, early), chunks = refs[:5], refs[5 : 5 + 2 * zs]
    gate_out, up_out, left = refs[5 + 2 * zs :]
    width = one.shape[0]
    left[:, :width] = one[...].T
    left[:, width:] = two[...].T
    order = chunks[0::2] + chunks[1::2]

    def body(at):
        hid_grad = early[:, at] + jnp.dot(
            left[...], stacked(order, at), preferred_element_type=jnp.float32
        )
        gate = gate_ref[:, at].astype(jnp.float32)
        up_val = up_ref[:, at].astype(jnp.float32)
        sig = jax.nn.sigmoid(gate)
        gate_out[:, at] = (
            hid_grad * up_val * sig * (1.0 + gate * (1.0 - sig))
        ).astype(jnp.bfloat16)
        up_out[:, at] = (hid_grad * gate * sig).astype(jnp.bfloat16)

    each_tile(gate_out.shape[1], body)


def merge_kernel(zs, rows, me_ref, *refs):
    parts, out, placed = refs[:4], refs[4], refs[5]
    me = me_ref[0]
    for far in range(2):
        value = parts[2 * far][...] + parts[2 * far + 1][...]
        for s in range(zs // 2):
            for core in range(2):
                block = me ^ (4 * s + 2 * far + core)
                start = pl.multiple_of((block % (2 * zs)) * rows, rows)
                first = (2 * s + core) * rows
                placed[pl.ds(start, rows), :] = value[first : first + rows, :]
    out[...] = placed[...].T.astype(out.dtype)


def adamw_kernel(zs, total, *refs):
    pieces, states, outs = refs[: 2 * zs], refs[2 * zs : 2 * zs + 3], refs[2 * zs + 3 :]
    base = 0
    for p in range(2):
        own, others = pieces[p * zs], pieces[p * zs + 1 : (p + 1) * zs]
        at = slice(base, base + own.shape[1])
        base = at.stop
        grad = own[...]
        for other in others:
            grad = grad + other[...].astype(jnp.float32)
        for out, value in zip(
            outs, adamw(grad / jnp.float32(total), *[state[:, at] for state in states])
        ):
            out[:, at] = value


def estimate(flops, moved):
    return pl.CostEstimate(flops=int(flops), bytes_accessed=int(moved), transcendentals=0)


def call(kernel, outs, ins, scratch=(), smem=0, flops=0):
    moved = sum(v.size * v.dtype.itemsize for v in list(ins) + list(outs))
    return pl.pallas_call(
        kernel,
        out_shape=list(outs),
        in_specs=[SMEM] * smem + [VMEM] * (len(ins) - smem),
        out_specs=[VMEM] * len(outs),
        scratch_shapes=list(scratch),
        compiler_params=pltpu.CompilerParams(vmem_limit_bytes=24 << 20),
        cost_estimate=estimate(flops, moved),
    )(*ins)


def direct(gate_pre, up_pre, out_grad, master, moment_one, moment_two):
    n = lax.axis_size("dp")
    zs = n // 4
    micro, span, width = gate_pre.shape
    tokens = micro * span
    depth = out_grad.shape[2]
    rows = master.shape[0]
    total = micro * span * n
    me_arr = jnp.full((1,), lax.axis_index("dp"), jnp.int32)
    rep_arr = jnp.full((1,), lax.axis_index("rep"), jnp.int32)
    tiles = width // TILE
    cuts = [0, (tiles + 1) // 2 * TILE, width]
    spread = range(1, zs)

    def swap(value, m):
        return lax.ppermute(value, "dp", [(i, i ^ m) for i in range(n)])

    def bf16(*shape):
        return jax.ShapeDtypeStruct(shape, jnp.bfloat16)

    def f32(*shape):
        return jax.ShapeDtypeStruct(shape, jnp.float32)

    gate = gate_pre.reshape(tokens, width)
    up_val = up_pre.reshape(tokens, width)
    cotangent = out_grad.reshape(tokens, depth)

    chunk = {0: lax.optimization_barrier(master.astype(jnp.bfloat16))}
    for s in spread:
        chunk[4 * s] = swap(chunk[0], 4 * s)
    for s in range(zs):
        chunk[4 * s + 2] = swap(chunk[4 * s], 2)
    for s in range(zs):
        chunk[4 * s + 1] = swap(chunk[4 * s], 1)
        chunk[4 * s + 3] = swap(chunk[4 * s + 2], 1)

    picked = call(
        functools.partial(select_kernel, zs, rows),
        [bf16(zs * rows, tokens)] * 4,
        [me_arr, cotangent],
        [pltpu.VMEM((depth, tokens), jnp.bfloat16)],
        smem=1,
    )
    lefts = [picked[0]] + [swap(picked[m], m) for m in range(1, 4)]
    hidden, sums = [], []
    for lo, hi in zip(cuts[:-1], cuts[1:]):
        own = gated(gate[:, lo:hi], up_val[:, lo:hi])
        hidden.append(own)
        across = swap(own, 2)
        rights = [own, swap(own, 1), across, swap(across, 1)]
        size = hi - lo
        parts = call(
            functools.partial(grads_kernel, zs, rows),
            [f32(rows, size)] + [bf16(rows, size)] * (zs - 1),
            lefts + rights,
            flops=8 * zs * rows * tokens * size,
        )
        sums.extend([parts[0]] + [swap(parts[s], 4 * s) for s in spread])
    turned = call(turn_kernel, [bf16(h.shape[1], tokens) for h in hidden], hidden)

    near = [chunk[4 * s + m] for s in range(zs) for m in (0, 1)]
    far = [chunk[4 * s + m] for s in range(zs) for m in (2, 3)]
    deep, half = depth // 2, depth // 4
    work = 2 * tokens * deep * width
    left = [pltpu.VMEM((tokens, deep), jnp.bfloat16)]
    product = [pltpu.VMEM((deep, tokens), jnp.float32)]
    keep_near, send_near, early = call(
        functools.partial(near_kernel, zs),
        [f32(half, tokens), f32(half, tokens), f32(tokens, width)],
        [me_arr, rep_arr, *turned, picked[0], picked[1], *near],
        left + product,
        smem=2,
        flops=2 * work,
    )

    def across_rep(value):
        return lax.ppermute(value, "rep", [(0, 1), (1, 0)])

    got_near = across_rep(send_near)
    keep_far, send_far = call(
        functools.partial(far_kernel, zs),
        [f32(half, tokens), f32(half, tokens)],
        [me_arr, rep_arr, *turned, *far],
        product,
        smem=2,
        flops=work,
    )
    got_far = across_rep(send_far)
    gate_grad, up_grad = call(
        functools.partial(back_kernel, zs),
        [bf16(tokens, width)] * 2,
        [picked[2], picked[3], gate, up_val, early, *far],
        left,
        flops=work,
    )
    (out,) = call(
        functools.partial(merge_kernel, zs, rows),
        [bf16(tokens, 2 * half)],
        [me_arr, keep_near, got_near, keep_far, got_far],
        [pltpu.VMEM((2 * half, tokens), jnp.float32)],
        smem=1,
    )
    master_new, first, second = call(
        functools.partial(adamw_kernel, zs, total),
        [f32(rows, width)] * 3,
        sums + [master, moment_one, moment_two],
    )
    return (
        out.reshape(micro, span, 2 * half),
        gate_grad.reshape(gate_pre.shape),
        up_grad.reshape(gate_pre.shape),
        master_new,
        first,
        second,
    )


def small(n, reps, width):
    return n == 16 and reps == 2 and width % TILE == 0


def on_device(gate_pre, *rest):
    if small(lax.axis_size("dp"), lax.axis_size("rep"), gate_pre.shape[2]):
        return direct(gate_pre, *rest)
    return plain(gate_pre, *rest)


def solution(mesh):
    placed = (
        P(None, "dp", "rep"),
        P(None, "dp", "rep"),
        P(None, "dp", None),
        P("dp", "rep"),
        P("dp", "rep"),
        P("dp", "rep"),
    )
    return jax.shard_map(
        on_device,
        mesh=mesh,
        in_specs=placed,
        out_specs=(
            P(None, "dp", "rep"),
            P(None, "dp", "rep"),
            P(None, "dp", "rep"),
            P("dp", "rep"),
            P("dp", "rep"),
            P("dp", "rep"),
        ),
        check_vma=False,
    )
```

```python
import functools
import jax
import jax.numpy as jnp
from jax import lax
from jax.experimental import pallas as pl
from jax.experimental.pallas import tpu as pltpu
from jax.sharding import PartitionSpec as P


first_power = 2.6561398887587544e-05
second_power = 0.005920529220333997


VMEM = pl.BlockSpec(memory_space=pltpu.VMEM)
SMEM = pl.BlockSpec(memory_space=pltpu.SMEM)
TILE = 256


def adamw(main_grad, master, moment_one, moment_two):
    first = 0.9 * moment_one + 0.1 * main_grad
    second = 0.95 * moment_two + 0.05 * main_grad * main_grad
    update = first / (1.0 - first_power) / (jnp.sqrt(second / (1.0 - second_power)) + 1e-08)
    return master - 0.003 * (update + 0.1 * master), first, second


def gated(gate, up_val):
    gate = gate.astype(jnp.float32)
    return (gate * jax.nn.sigmoid(gate) * up_val.astype(jnp.float32)).astype(jnp.bfloat16)


def plain(gate_pre, up_pre, out_grad, master, moment_one, moment_two):
    micro, rows, width = gate_pre.shape
    total = micro * rows * lax.axis_size("dp")
    weights = lax.all_gather(master.astype(jnp.bfloat16), "dp", axis=0, tiled=True)
    hidden = gated(gate_pre, up_pre).reshape(-1, width)
    cotangent = out_grad.reshape(-1, out_grad.shape[2])
    grads = lax.dot_general(
        cotangent, hidden, (((0,), (0,)), ((), ())), preferred_element_type=jnp.float32
    )
    part = lax.dot_general(
        hidden, weights, (((1,), (1,)), ((), ())), preferred_element_type=jnp.float32
    )
    hid_grad = jnp.dot(cotangent, weights, preferred_element_type=jnp.float32)
    grads = lax.psum_scatter(grads, "dp", scatter_dimension=0, tiled=True)
    out = lax.psum_scatter(part, "rep", scatter_dimension=1, tiled=True).astype(jnp.bfloat16)
    gate = gate_pre.reshape(-1, width).astype(jnp.float32)
    up_val = up_pre.reshape(-1, width).astype(jnp.float32)
    sig = jax.nn.sigmoid(gate)
    gate_grad = (hid_grad * up_val * sig * (1.0 + gate * (1.0 - sig))).astype(jnp.bfloat16)
    up_grad = (hid_grad * gate * sig).astype(jnp.bfloat16)
    master_new, first, second = adamw(
        grads / jnp.float32(total), master, moment_one, moment_two
    )
    return (
        out.reshape(micro, rows, -1),
        gate_grad.reshape(gate_pre.shape),
        up_grad.reshape(gate_pre.shape),
        master_new,
        first,
        second,
    )


def select_kernel(zs, rows, me_ref, rep_ref, og_ref, own, near, far, rest, turned):
    turned[...] = og_ref[...].T
    me, rep = me_ref[0], rep_ref[0]

    def block(s, m):
        start = pl.multiple_of((me ^ (4 * s) ^ m) * rows, rows)
        return turned[pl.ds(start, rows), :]

    for s in range(zs):
        own[s * rows : (s + 1) * rows, :] = block(s, 0)
        near[s * rows : (s + 1) * rows, :] = block(s, 1)
    for m in (2, 3):
        for i in range(zs // 2):
            first = ((m - 2) * (zs // 2) + i) * rows
            far[first : first + rows, :] = block(rep * (zs // 2) + i, m)
        for s in range(zs):
            first = ((m - 2) * zs + s) * rows
            rest[first : first + rows, :] = block(s, m)


def turn_kernel(first, second, own, near, rest, first_t, second_t, left_near, left_far):
    first_t[...] = first[...].T
    second_t[...] = second[...].T
    width = own.shape[0]
    left_near[:, :width] = own[...].T
    left_near[:, width:] = near[...].T
    left_far[...] = rest[...].T


def each_tile(width, body):
    for start in range(0, width, TILE):
        body(slice(start, start + TILE))


def grads_kernel(zs, rows, rep_ref, *refs):
    own, near, far, far_x, cross, cross_x = refs[:6]
    rights, outs, left = refs[6:10], refs[10 : 10 + zs], refs[10 + zs]
    count = own.shape[1]
    half = zs * rows // 2
    mine = pl.ds(pl.multiple_of(rep_ref[0] * half, half), half)
    other = pl.ds(pl.multiple_of((1 - rep_ref[0]) * half, half), half)
    left[:, :count] = own[...]
    left[:, count : 2 * count] = near[...]
    left[mine, 2 * count : 3 * count] = far[:half, :]
    left[other, 2 * count : 3 * count] = far_x[:half, :]
    left[mine, 3 * count :] = cross[half:, :]
    left[other, 3 * count :] = cross_x[half:, :]

    def body(at):
        total = jnp.dot(left[...], stacked(rights, at), preferred_element_type=jnp.float32)
        for s in range(zs):
            outs[s][:, at] = total[s * rows : (s + 1) * rows, :].astype(outs[s].dtype)

    each_tile(rights[0].shape[1], body)


def stacked(chunks, at):
    return jnp.concatenate([chunk[:, at] for chunk in chunks], axis=0)


def out_rows(zs, me_ref, rep_ref, turned, chunks, keep, send, total):
    base, value = 0, None
    for piece in turned:
        at = slice(base, base + piece.shape[0])
        term = jnp.dot(stacked(chunks, at), piece[...], preferred_element_type=jnp.float32)
        value = term if value is None else value + term
        base = at.stop
    total[...] = value
    half = keep.shape[0]
    flip = ((me_ref[0] // (2 * zs)) ^ rep_ref[0]) & 1
    keep[...] = total[pl.ds(pl.multiple_of(flip * half, half), half), :]
    send[...] = total[pl.ds(pl.multiple_of((1 - flip) * half, half), half), :]


def near_kernel(zs, me_ref, rep_ref, *refs):
    turned, left, chunks = refs[:2], refs[2], refs[3 : 3 + 2 * zs]
    keep, send, early, total = refs[3 + 2 * zs :]
    out_rows(zs, me_ref, rep_ref, turned, chunks, keep, send, total)
    order = chunks[0::2] + chunks[1::2]

    def body(at):
        early[:, at] = jnp.dot(
            left[...], stacked(order, at), preferred_element_type=jnp.float32
        )

    each_tile(early.shape[1], body)


def far_kernel(zs, me_ref, rep_ref, *refs):
    turned, chunks = refs[:2], refs[2 : 2 + 2 * zs]
    keep, send, total = refs[2 + 2 * zs :]
    out_rows(zs, me_ref, rep_ref, turned, chunks, keep, send, total)


def back_kernel(zs, left, gate_ref, up_ref, early, *refs):
    chunks, (gate_out, up_out) = refs[: 2 * zs], refs[2 * zs :]
    order = chunks[0::2] + chunks[1::2]

    def body(at):
        hid_grad = early[:, at] + jnp.dot(
            left[...], stacked(order, at), preferred_element_type=jnp.float32
        )
        gate = gate_ref[:, at].astype(jnp.float32)
        up_val = up_ref[:, at].astype(jnp.float32)
        sig = jax.nn.sigmoid(gate)
        gate_out[:, at] = (
            hid_grad * up_val * sig * (1.0 + gate * (1.0 - sig))
        ).astype(jnp.bfloat16)
        up_out[:, at] = (hid_grad * gate * sig).astype(jnp.bfloat16)

    each_tile(gate_out.shape[1], body)


def merge_kernel(zs, rows, me_ref, *refs):
    parts, out, placed = refs[:4], refs[4], refs[5]
    me = me_ref[0]
    for far in range(2):
        value = parts[2 * far][...] + parts[2 * far + 1][...]
        for s in range(zs // 2):
            for core in range(2):
                block = me ^ (4 * s + 2 * far + core)
                start = pl.multiple_of((block % (2 * zs)) * rows, rows)
                first = (2 * s + core) * rows
                placed[pl.ds(start, rows), :] = value[first : first + rows, :]
    out[...] = placed[...].T.astype(out.dtype)


def adamw_kernel(zs, total, *refs):
    pieces, states, outs = refs[: 2 * zs], refs[2 * zs : 2 * zs + 3], refs[2 * zs + 3 :]
    base = 0
    for p in range(2):
        own, others = pieces[p * zs], pieces[p * zs + 1 : (p + 1) * zs]
        at = slice(base, base + own.shape[1])
        base = at.stop
        grad = own[...]
        for other in others:
            grad = grad + other[...].astype(jnp.float32)
        for out, value in zip(
            outs, adamw(grad / jnp.float32(total), *[state[:, at] for state in states])
        ):
            out[:, at] = value


def estimate(flops, moved):
    return pl.CostEstimate(flops=int(flops), bytes_accessed=int(moved), transcendentals=0)


def call(kernel, outs, ins, scratch=(), smem=0, flops=0):
    moved = sum(v.size * v.dtype.itemsize for v in list(ins) + list(outs))
    return pl.pallas_call(
        kernel,
        out_shape=list(outs),
        in_specs=[SMEM] * smem + [VMEM] * (len(ins) - smem),
        out_specs=[VMEM] * len(outs),
        scratch_shapes=list(scratch),
        compiler_params=pltpu.CompilerParams(vmem_limit_bytes=24 << 20),
        cost_estimate=estimate(flops, moved),
    )(*ins)


def direct(gate_pre, up_pre, out_grad, master, moment_one, moment_two):
    n = lax.axis_size("dp")
    zs = n // 4
    micro, span, width = gate_pre.shape
    tokens = micro * span
    depth = out_grad.shape[2]
    rows = master.shape[0]
    total = micro * span * n
    me_arr = jnp.full((1,), lax.axis_index("dp"), jnp.int32)
    rep_arr = jnp.full((1,), lax.axis_index("rep"), jnp.int32)
    tiles = width // TILE
    cuts = [0, (tiles + 1) // 2 * TILE, width]
    spread = range(1, zs)

    def swap(value, m):
        return lax.ppermute(value, "dp", [(i, i ^ m) for i in range(n)])

    def bf16(*shape):
        return jax.ShapeDtypeStruct(shape, jnp.bfloat16)

    def f32(*shape):
        return jax.ShapeDtypeStruct(shape, jnp.float32)

    gate = gate_pre.reshape(tokens, width)
    up_val = up_pre.reshape(tokens, width)
    cotangent = out_grad.reshape(tokens, depth)

    chunk = {0: lax.optimization_barrier(master.astype(jnp.bfloat16))}
    chunk[2] = swap(chunk[0], 2)
    chunk[4] = swap(chunk[0], 4)
    chunk[8] = swap(chunk[0], 8)
    chunk[12] = swap(chunk[8], 4)
    chunk[6] = swap(chunk[2], 4)
    chunk[10] = swap(chunk[8], 2)
    chunk[14] = swap(chunk[12], 2)
    for s in range(zs):
        chunk[4 * s + 1] = swap(chunk[4 * s], 1)
        chunk[4 * s + 3] = swap(chunk[4 * s + 2], 1)

    def across_rep(value):
        return lax.ppermute(value, "rep", [(0, 1), (1, 0)])

    picked = call(
        functools.partial(select_kernel, zs, rows),
        [bf16(zs * rows, tokens)] * 3 + [bf16(2 * zs * rows, tokens)],
        [me_arr, rep_arr, cotangent],
        [pltpu.VMEM((depth, tokens), jnp.bfloat16)],
        smem=2,
    )
    far_half = swap(picked[2], 2)
    far_rest = across_rep(far_half)
    lefts = [
        picked[0],
        swap(picked[1], 1),
        far_half,
        far_rest,
        swap(far_half, 1),
        swap(far_rest, 1),
    ]
    hidden, sums = [], []
    for lo, hi in zip(cuts[:-1], cuts[1:]):
        own = gated(gate[:, lo:hi], up_val[:, lo:hi])
        hidden.append(own)
        across = swap(own, 2)
        rights = [own, swap(own, 1), across, swap(across, 1)]
        size = hi - lo
        parts = call(
            functools.partial(grads_kernel, zs, rows),
            [f32(rows, size)] + [bf16(rows, size)] * (zs - 1),
            [rep_arr] + lefts + rights,
            [pltpu.VMEM((zs * rows, 4 * tokens), jnp.bfloat16)],
            smem=1,
            flops=8 * zs * rows * tokens * size,
        )
        sums.extend([parts[0]] + [swap(parts[s], 4 * s) for s in spread])
    first_t, second_t, left_near, left_far = call(
        turn_kernel,
        [bf16(h.shape[1], tokens) for h in hidden] + [bf16(tokens, depth // 2)] * 2,
        hidden + [picked[0], picked[1], picked[3]],
    )
    turned = [first_t, second_t]

    near = [chunk[4 * s + m] for s in range(zs) for m in (0, 1)]
    far = [chunk[4 * s + m] for s in range(zs) for m in (2, 3)]
    deep, half = depth // 2, depth // 4
    work = 2 * tokens * deep * width
    product = [pltpu.VMEM((deep, tokens), jnp.float32)]
    keep_near, send_near, early = call(
        functools.partial(near_kernel, zs),
        [f32(half, tokens), f32(half, tokens), f32(tokens, width)],
        [me_arr, rep_arr, *turned, left_near, *near],
        product,
        smem=2,
        flops=2 * work,
    )

    got_near = across_rep(send_near)
    keep_far, send_far = call(
        functools.partial(far_kernel, zs),
        [f32(half, tokens), f32(half, tokens)],
        [me_arr, rep_arr, *turned, *far],
        product,
        smem=2,
        flops=work,
    )
    got_far = across_rep(send_far)
    gate_grad, up_grad = call(
        functools.partial(back_kernel, zs),
        [bf16(tokens, width)] * 2,
        [left_far, gate, up_val, early, *far],
        flops=work,
    )
    (out,) = call(
        functools.partial(merge_kernel, zs, rows),
        [bf16(tokens, 2 * half)],
        [me_arr, keep_near, got_near, keep_far, got_far],
        [pltpu.VMEM((2 * half, tokens), jnp.float32)],
        smem=1,
    )
    master_new, first, second = call(
        functools.partial(adamw_kernel, zs, total),
        [f32(rows, width)] * 3,
        sums + [master, moment_one, moment_two],
    )
    return (
        out.reshape(micro, span, 2 * half),
        gate_grad.reshape(gate_pre.shape),
        up_grad.reshape(gate_pre.shape),
        master_new,
        first,
        second,
    )


def small(n, reps, width):
    return n == 16 and reps == 2 and width % TILE == 0


def on_device(gate_pre, *rest):
    if small(lax.axis_size("dp"), lax.axis_size("rep"), gate_pre.shape[2]):
        return direct(gate_pre, *rest)
    return plain(gate_pre, *rest)


def solution(mesh):
    placed = (
        P(None, "dp", "rep"),
        P(None, "dp", "rep"),
        P(None, "dp", None),
        P("dp", "rep"),
        P("dp", "rep"),
        P("dp", "rep"),
    )
    return jax.shard_map(
        on_device,
        mesh=mesh,
        in_specs=placed,
        out_specs=(
            P(None, "dp", "rep"),
            P(None, "dp", "rep"),
            P(None, "dp", "rep"),
            P("dp", "rep"),
            P("dp", "rep"),
            P("dp", "rep"),
        ),
        check_vma=False,
    )
```

```python
import functools
import jax
import jax.numpy as jnp
from jax import lax
from jax.experimental import pallas as pl
from jax.experimental.pallas import tpu as pltpu
from jax.sharding import PartitionSpec as P


first_power = 2.6561398887587544e-05
second_power = 0.005920529220333997


VMEM = pl.BlockSpec(memory_space=pltpu.VMEM)
SMEM = pl.BlockSpec(memory_space=pltpu.SMEM)
TILE = 256


def adamw(main_grad, master, moment_one, moment_two):
    first = 0.9 * moment_one + 0.1 * main_grad
    second = 0.95 * moment_two + 0.05 * main_grad * main_grad
    update = first / (1.0 - first_power) / (jnp.sqrt(second / (1.0 - second_power)) + 1e-08)
    return master - 0.003 * (update + 0.1 * master), first, second


def gated(gate, up_val):
    gate = gate.astype(jnp.float32)
    return (gate * jax.nn.sigmoid(gate) * up_val.astype(jnp.float32)).astype(jnp.bfloat16)


def plain(gate_pre, up_pre, out_grad, master, moment_one, moment_two):
    micro, rows, width = gate_pre.shape
    total = micro * rows * lax.axis_size("dp")
    weights = lax.all_gather(master.astype(jnp.bfloat16), "dp", axis=0, tiled=True)
    hidden = gated(gate_pre, up_pre).reshape(-1, width)
    cotangent = out_grad.reshape(-1, out_grad.shape[2])
    grads = lax.dot_general(
        cotangent, hidden, (((0,), (0,)), ((), ())), preferred_element_type=jnp.float32
    )
    part = lax.dot_general(
        hidden, weights, (((1,), (1,)), ((), ())), preferred_element_type=jnp.float32
    )
    hid_grad = jnp.dot(cotangent, weights, preferred_element_type=jnp.float32)
    grads = lax.psum_scatter(grads, "dp", scatter_dimension=0, tiled=True)
    out = lax.psum_scatter(part, "rep", scatter_dimension=1, tiled=True).astype(jnp.bfloat16)
    gate = gate_pre.reshape(-1, width).astype(jnp.float32)
    up_val = up_pre.reshape(-1, width).astype(jnp.float32)
    sig = jax.nn.sigmoid(gate)
    gate_grad = (hid_grad * up_val * sig * (1.0 + gate * (1.0 - sig))).astype(jnp.bfloat16)
    up_grad = (hid_grad * gate * sig).astype(jnp.bfloat16)
    master_new, first, second = adamw(
        grads / jnp.float32(total), master, moment_one, moment_two
    )
    return (
        out.reshape(micro, rows, -1),
        gate_grad.reshape(gate_pre.shape),
        up_grad.reshape(gate_pre.shape),
        master_new,
        first,
        second,
    )


def select_kernel(zs, rows, me_ref, rep_ref, og_ref, own, near, far, rest, turned):
    turned[...] = og_ref[...].T
    me, rep = me_ref[0], rep_ref[0]

    def block(s, m):
        start = pl.multiple_of((me ^ (4 * s) ^ m) * rows, rows)
        return turned[pl.ds(start, rows), :]

    for s in range(zs):
        own[s * rows : (s + 1) * rows, :] = block(s, 0)
        near[s * rows : (s + 1) * rows, :] = block(s, 1)
    for m in (2, 3):
        for i in range(zs // 2):
            first = ((m - 2) * (zs // 2) + i) * rows
            far[first : first + rows, :] = block(rep * (zs // 2) + i, m)
        for s in range(zs):
            first = ((m - 2) * zs + s) * rows
            rest[first : first + rows, :] = block(s, m)


def turn_kernel(count, *refs):
    hidden, (own, near, rest) = refs[:count], refs[count : count + 3]
    turned, (left_near, left_far) = refs[count + 3 : 2 * count + 3], refs[2 * count + 3 :]
    for source, target in zip(hidden, turned):
        target[...] = source[...].T
    width = own.shape[0]
    left_near[:, :width] = own[...].T
    left_near[:, width:] = near[...].T
    left_far[...] = rest[...].T


def each_tile(width, body):
    for start in range(0, width, TILE):
        body(slice(start, start + TILE))


def grads_kernel(rows, rep_ref, *refs):
    own, near, far, far_x, cross, cross_x = refs[:6]
    rights, (mine_out, side, across, left) = refs[6:10], refs[10:]
    count = own.shape[1]
    half = 2 * rows
    mine = pl.ds(pl.multiple_of(rep_ref[0] * half, half), half)
    other = pl.ds(pl.multiple_of((1 - rep_ref[0]) * half, half), half)
    left[:, :count] = own[...]
    left[:, count : 2 * count] = near[...]
    left[mine, 2 * count : 3 * count] = far[:half, :]
    left[other, 2 * count : 3 * count] = far_x[:half, :]
    left[mine, 3 * count :] = cross[half:, :]
    left[other, 3 * count :] = cross_x[half:, :]

    def body(at):
        total = jnp.dot(left[...], stacked(rights, at), preferred_element_type=jnp.float32)
        mine_out[:, at] = total[:rows]
        side[:rows, at] = total[rows : 2 * rows].astype(side.dtype)
        side[rows:, at] = total[3 * rows :].astype(side.dtype)
        across[:, at] = total[2 * rows : 3 * rows]

    each_tile(rights[0].shape[1], body)


def add_kernel(across, side, out):
    rows = across.shape[0]
    out[...] = (across[...] + side[rows:, :].astype(jnp.float32)).astype(out.dtype)


def stacked(chunks, at):
    return jnp.concatenate([chunk[:, at] for chunk in chunks], axis=0)


def flipped(zs, me_ref, rep_ref):
    return ((me_ref[0] // (2 * zs)) ^ rep_ref[0]) & 1


def out_rows(turned, chunks):
    base, value = 0, None
    for piece in turned:
        at = slice(base, base + piece.shape[0])
        term = jnp.dot(stacked(chunks, at), piece[...], preferred_element_type=jnp.float32)
        value = term if value is None else value + term
        base = at.stop
    return value


def back_term(left, chunks, at):
    order = chunks[0::2] + chunks[1::2]
    return jnp.dot(left[...], stacked(order, at), preferred_element_type=jnp.float32)


def near_kernel(zs, pieces, me_ref, rep_ref, *refs):
    turned, left, chunks = refs[:pieces], refs[pieces], refs[pieces + 1 : pieces + 1 + 2 * zs]
    keep, send, early, total = refs[pieces + 1 + 2 * zs :]
    total[...] = out_rows(turned, chunks)
    half = keep.shape[0]
    flip = flipped(zs, me_ref, rep_ref)
    keep[...] = total[pl.ds(pl.multiple_of(flip * half, half), half), :]
    send[...] = total[pl.ds(pl.multiple_of((1 - flip) * half, half), half), :]

    def body(at):
        early[:, at] = back_term(left, chunks, at)

    each_tile(early.shape[1], body)


def middle_kernel(zs, pieces, me_ref, rep_ref, *refs):
    turned, chunks = refs[:pieces], refs[pieces : pieces + 2 * (zs - 1)]
    keep, send, hold = refs[pieces + 2 * (zs - 1) :]
    value = out_rows(turned, chunks)
    span = keep.shape[0]
    flip = flipped(zs, me_ref, rep_ref)
    hold[...] = value[span : 2 * span]

    @pl.when(flip == 0)
    def _():
        keep[...] = value[:span]
        send[...] = value[2 * span :]

    @pl.when(flip == 1)
    def _():
        keep[...] = value[2 * span :]
        send[...] = value[:span]


def last_kernel(zs, pieces, me_ref, rep_ref, *refs):
    turned, (hold, one, two, keep, send) = refs[:pieces], refs[pieces:]
    value = out_rows(turned, (one, two))
    flip = flipped(zs, me_ref, rep_ref)

    @pl.when(flip == 0)
    def _():
        keep[...] = hold[...]
        send[...] = value

    @pl.when(flip == 1)
    def _():
        keep[...] = value
        send[...] = hold[...]


def store_tile(index, at, sems, pairs):
    copies = []
    for k, (source, target) in enumerate(pairs):
        copy = pltpu.make_async_copy(
            source.at[:, at], target.at[:, at], sems.at[index * len(pairs) + k]
        )
        copy.start()
        copies.append(copy)
    return copies


def slopes_kernel(gate_ref, up_ref, gate_slope, up_slope):
    def body(at):
        gate = gate_ref[:, at].astype(jnp.float32)
        sig = jax.nn.sigmoid(gate)
        gate_slope[:, at] = up_ref[:, at].astype(jnp.float32) * sig * (1.0 + gate * (1.0 - sig))
        up_slope[:, at] = gate * sig

    each_tile(gate_ref.shape[1], body)


def back_kernel(zs, left, gate_slope, up_slope, early, *refs):
    chunks, (gate_out, up_out, gate_tiles, up_tiles, sems) = refs[: 2 * zs], refs[2 * zs :]
    copies = []

    def body(at):
        hid_grad = early[:, at] + back_term(left, chunks, at)
        gate_tiles[:, at] = (hid_grad * gate_slope[:, at]).astype(jnp.bfloat16)
        up_tiles[:, at] = (hid_grad * up_slope[:, at]).astype(jnp.bfloat16)
        pairs = ((gate_tiles, gate_out), (up_tiles, up_out))
        copies.extend(store_tile(len(copies) // 2, at, sems, pairs))

    each_tile(gate_out.shape[1], body)
    for copy in copies:
        copy.wait()


def merge_kernel(zs, rows, me_ref, *refs):
    keep, got, middle, got_middle, last, got_last, out, placed = refs
    me = me_ref[0]

    def place(value, first, far):
        for s in range(value.shape[0] // (2 * rows)):
            for core in range(2):
                block = me ^ (4 * (first + s) + 2 * far + core)
                start = pl.multiple_of((block % (2 * zs)) * rows, rows)
                at = (2 * s + core) * rows
                placed[pl.ds(start, rows), :] = value[at : at + rows, :]

    place(keep[...] + got[...], 0, 0)
    place(middle[...] + got_middle[...], 0, 1)
    place(last[...] + got_last[...], 1, 1)
    out[...] = placed[...].T.astype(out.dtype)


def adamw_kernel(total, pieces, *refs):
    parts, states = refs[: 3 * pieces], refs[3 * pieces : 3 * pieces + 3]
    outs, values, sems = refs[3 * pieces + 3 :][:3], refs[3 * pieces + 6 : -1], refs[-1]
    rows = outs[0].shape[0]
    base, copies = 0, []
    for p in range(pieces):
        own, side, passed = parts[3 * p : 3 * p + 3]
        at = slice(base, base + own.shape[1])
        base = at.stop
        grad = own[...] + side[:rows, :].astype(jnp.float32) + passed[...].astype(jnp.float32)
        results = adamw(grad / jnp.float32(total), *[state[:, at] for state in states])
        for tile, value in zip(values, results):
            tile[:, at] = value
        copies.extend(store_tile(p, at, sems, tuple(zip(values, outs))))
    for copy in copies:
        copy.wait()


def estimate(flops, moved):
    return pl.CostEstimate(flops=int(flops), bytes_accessed=int(moved), transcendentals=0)


def call(kernel, outs, ins, scratch=(), smem=0, flops=0, copied=False):
    moved = sum(v.size * v.dtype.itemsize for v in list(ins) + list(outs))
    return pl.pallas_call(
        kernel,
        out_shape=list(outs),
        in_specs=[SMEM] * smem + [VMEM] * (len(ins) - smem),
        out_specs=[pl.BlockSpec(memory_space=pl.ANY) if copied else VMEM] * len(outs),
        scratch_shapes=list(scratch),
        compiler_params=pltpu.CompilerParams(vmem_limit_bytes=24 << 20),
        cost_estimate=estimate(flops, moved),
    )(*ins)


def direct(gate_pre, up_pre, out_grad, master, moment_one, moment_two):
    n = lax.axis_size("dp")
    zs = n // 4
    micro, span, width = gate_pre.shape
    tokens = micro * span
    depth = out_grad.shape[2]
    rows = master.shape[0]
    total = micro * span * n
    me_arr = jnp.full((1,), lax.axis_index("dp"), jnp.int32)
    rep_arr = jnp.full((1,), lax.axis_index("rep"), jnp.int32)
    tiles = width // TILE
    pieces = len(SHARES)
    cuts = [tiles * sum(SHARES[:p]) // sum(SHARES) * TILE for p in range(pieces + 1)]

    def swap(value, m):
        return lax.ppermute(value, "dp", [(i, i ^ m) for i in range(n)])

    def bf16(*shape):
        return jax.ShapeDtypeStruct(shape, jnp.bfloat16)

    def f32(*shape):
        return jax.ShapeDtypeStruct(shape, jnp.float32)

    gate = gate_pre.reshape(tokens, width)
    up_val = up_pre.reshape(tokens, width)
    cotangent = out_grad.reshape(tokens, depth)

    chunk = {0: lax.optimization_barrier(master.astype(jnp.bfloat16))}
    chunk[2] = swap(chunk[0], 2)
    chunk[4] = swap(chunk[0], 4)
    chunk[8] = swap(chunk[0], 8)
    chunk[12] = swap(chunk[8], 4)
    chunk[6] = swap(chunk[2], 4)
    chunk[10] = swap(chunk[8], 2)
    chunk[14] = swap(chunk[12], 2)
    for s in range(zs):
        chunk[4 * s + 1] = swap(chunk[4 * s], 1)
        chunk[4 * s + 3] = swap(chunk[4 * s + 2], 1)

    def across_rep(value):
        return lax.ppermute(value, "rep", [(0, 1), (1, 0)])

    picked = call(
        functools.partial(select_kernel, zs, rows),
        [bf16(zs * rows, tokens)] * 3 + [bf16(2 * zs * rows, tokens)],
        [me_arr, rep_arr, cotangent],
        [pltpu.VMEM((depth, tokens), jnp.bfloat16)],
        smem=2,
    )
    far_half = swap(picked[2], 2)
    far_rest = across_rep(far_half)
    lefts = [
        picked[0], swap(picked[1], 1), far_half, far_rest, swap(far_half, 1), swap(far_rest, 1)
    ]
    hidden, sums = [], []
    for lo, hi in zip(cuts[:-1], cuts[1:]):
        own = gated(gate[:, lo:hi], up_val[:, lo:hi])
        hidden.append(own)
        across = swap(own, 2)
        rights = [own, swap(own, 1), across, swap(across, 1)]
        size = hi - lo
        own_sum, side, across_sum = call(
            functools.partial(grads_kernel, rows),
            [f32(rows, size), bf16(2 * rows, size), f32(rows, size)],
            [rep_arr] + lefts + rights,
            [pltpu.VMEM((zs * rows, 4 * tokens), jnp.bfloat16)],
            smem=1,
            flops=8 * zs * rows * tokens * size,
        )
        side = swap(side, 4)
        (passed,) = call(add_kernel, [bf16(rows, size)], [across_sum, side])
        sums.extend([own_sum, side, swap(passed, 8)])
    *turned, left_near, left_far = call(
        functools.partial(turn_kernel, pieces),
        [bf16(h.shape[1], tokens) for h in hidden] + [bf16(tokens, depth // 2)] * 2,
        hidden + [picked[0], picked[1], picked[3]],
    )

    near = [chunk[4 * s + m] for s in range(zs) for m in (0, 1)]
    far = [chunk[4 * s + m] for s in range(zs) for m in (2, 3)]
    deep, half = depth // 2, depth // 4
    last = 2 * rows
    work = 2 * tokens * deep * width
    keep, send, early = call(
        functools.partial(near_kernel, zs, pieces),
        [f32(half, tokens), f32(half, tokens), f32(tokens, width)],
        [me_arr, rep_arr, *turned, left_near, *near],
        [pltpu.VMEM((deep, tokens), jnp.float32)],
        smem=2,
        flops=2 * work,
    )
    got = across_rep(send)
    middle, send_middle, hold = call(
        functools.partial(middle_kernel, zs, pieces),
        [f32(last, tokens)] * 3,
        [me_arr, rep_arr, *turned, *far[:-2]],
        smem=2,
        flops=work,
    )
    got_middle = across_rep(send_middle)
    keep_last, send_last = call(
        functools.partial(last_kernel, zs, pieces),
        [f32(last, tokens)] * 2,
        [me_arr, rep_arr, *turned, hold, *far[-2:]],
        smem=2,
        flops=work // zs,
    )
    got_last = across_rep(send_last)
    slopes = call(slopes_kernel, [f32(tokens, width)] * 2, [gate, up_val])
    gate_grad, up_grad = call(
        functools.partial(back_kernel, zs),
        [bf16(tokens, width)] * 2,
        [left_far, *slopes, early, *far],
        [pltpu.VMEM((tokens, width), jnp.bfloat16)] * 2 + [pltpu.SemaphoreType.DMA((2 * tiles,))],
        flops=work,
        copied=True,
    )
    (out,) = call(
        functools.partial(merge_kernel, zs, rows),
        [bf16(tokens, 2 * half)],
        [me_arr, keep, got, middle, got_middle, keep_last, got_last],
        [pltpu.VMEM((2 * half, tokens), jnp.float32)],
        smem=1,
    )
    master_new, first, second = call(
        functools.partial(adamw_kernel, total, pieces),
        [f32(rows, width)] * 3,
        sums + [master, moment_one, moment_two],
        [pltpu.VMEM((rows, width), jnp.float32)] * 3 + [pltpu.SemaphoreType.DMA((3 * pieces,))],
        copied=True,
    )
    return (
        out.reshape(micro, span, 2 * half),
        gate_grad.reshape(gate_pre.shape),
        up_grad.reshape(gate_pre.shape),
        master_new,
        first,
        second,
    )


SHARES = (4, 4, 3)


def small(n, reps, width):
    return n == 16 and reps == 2 and width % TILE == 0


def on_device(gate_pre, *rest):
    if small(lax.axis_size("dp"), lax.axis_size("rep"), gate_pre.shape[2]):
        return direct(gate_pre, *rest)
    return plain(gate_pre, *rest)


def solution(mesh):
    placed = (
        P(None, "dp", "rep"),
        P(None, "dp", "rep"),
        P(None, "dp", None),
        P("dp", "rep"),
        P("dp", "rep"),
        P("dp", "rep"),
    )
    return jax.shard_map(
        on_device,
        mesh=mesh,
        in_specs=placed,
        out_specs=(
            P(None, "dp", "rep"),
            P(None, "dp", "rep"),
            P(None, "dp", "rep"),
            P("dp", "rep"),
            P("dp", "rep"),
            P("dp", "rep"),
        ),
        check_vma=False,
    )
```

```python
import functools
import jax
import jax.numpy as jnp
from jax import lax
from jax.experimental import pallas as pl
from jax.experimental.pallas import tpu as pltpu
from jax.sharding import PartitionSpec as P


first_power = 2.6561398887587544e-05
second_power = 0.005920529220333997


VMEM = pl.BlockSpec(memory_space=pltpu.VMEM)
SMEM = pl.BlockSpec(memory_space=pltpu.SMEM)
TILE = 256


def adamw(main_grad, master, moment_one, moment_two):
    first = 0.9 * moment_one + 0.1 * main_grad
    second = 0.95 * moment_two + 0.05 * main_grad * main_grad
    scaled = first * (1.0 / (1.0 - first_power))
    update = scaled / (jnp.sqrt(second * (1.0 / (1.0 - second_power))) + 1e-08)
    return master - 0.003 * (update + 0.1 * master), first, second


def gated(gate, up_val):
    gate = gate.astype(jnp.float32)
    return (gate * jax.nn.sigmoid(gate) * up_val.astype(jnp.float32)).astype(jnp.bfloat16)


def plain(gate_pre, up_pre, out_grad, master, moment_one, moment_two):
    micro, rows, width = gate_pre.shape
    total = micro * rows * lax.axis_size("dp")
    weights = lax.all_gather(master.astype(jnp.bfloat16), "dp", axis=0, tiled=True)
    hidden = gated(gate_pre, up_pre).reshape(-1, width)
    cotangent = out_grad.reshape(-1, out_grad.shape[2])
    grads = lax.dot_general(
        cotangent, hidden, (((0,), (0,)), ((), ())), preferred_element_type=jnp.float32
    )
    part = lax.dot_general(
        hidden, weights, (((1,), (1,)), ((), ())), preferred_element_type=jnp.float32
    )
    hid_grad = jnp.dot(cotangent, weights, preferred_element_type=jnp.float32)
    grads = lax.psum_scatter(grads, "dp", scatter_dimension=0, tiled=True)
    out = lax.psum_scatter(part, "rep", scatter_dimension=1, tiled=True).astype(jnp.bfloat16)
    gate = gate_pre.reshape(-1, width).astype(jnp.float32)
    up_val = up_pre.reshape(-1, width).astype(jnp.float32)
    sig = jax.nn.sigmoid(gate)
    gate_grad = (hid_grad * up_val * sig * (1.0 + gate * (1.0 - sig))).astype(jnp.bfloat16)
    up_grad = (hid_grad * gate * sig).astype(jnp.bfloat16)
    master_new, first, second = adamw(
        grads / jnp.float32(total), master, moment_one, moment_two
    )
    return (
        out.reshape(micro, rows, -1),
        gate_grad.reshape(gate_pre.shape),
        up_grad.reshape(gate_pre.shape),
        master_new,
        first,
        second,
    )


def select_kernel(zs, rows, me_ref, rep_ref, og_ref, own, near, far, rest, turned):
    turned[...] = og_ref[...].T
    me, rep = me_ref[0], rep_ref[0]

    def block(s, m):
        start = pl.multiple_of((me ^ (4 * s) ^ m) * rows, rows)
        return turned[pl.ds(start, rows), :]

    for s in range(zs):
        own[s * rows : (s + 1) * rows, :] = block(s, 0)
        near[s * rows : (s + 1) * rows, :] = block(s, 1)
    for m in (2, 3):
        for i in range(zs // 2):
            first = ((m - 2) * (zs // 2) + i) * rows
            far[first : first + rows, :] = block(rep * (zs // 2) + i, m)
        for s in range(zs):
            first = ((m - 2) * zs + s) * rows
            rest[first : first + rows, :] = block(s, m)


def turn_kernel(count, *refs):
    hidden, (own, near, rest) = refs[:count], refs[count : count + 3]
    turned, (left_near, left_far) = refs[count + 3 : 2 * count + 3], refs[2 * count + 3 :]
    for source, target in zip(hidden, turned):
        target[...] = source[...].T
    width = own.shape[0]
    left_near[:, :width] = own[...].T
    left_near[:, width:] = near[...].T
    left_far[...] = rest[...].T


def each_tile(width, body):
    for start in range(0, width, TILE):
        body(slice(start, start + TILE))


def grads_kernel(rows, final, rep_ref, *refs):
    own, near, far, far_x, cross, cross_x = refs[:6]
    rights, (mine_out, side, across, *third), left = refs[6:10], refs[10:-1], refs[-1]
    count = own.shape[1]
    half = 2 * rows
    mine = pl.ds(pl.multiple_of(rep_ref[0] * half, half), half)
    other = pl.ds(pl.multiple_of((1 - rep_ref[0]) * half, half), half)
    left[:, :count] = own[...]
    left[:, count : 2 * count] = near[...]
    left[mine, 2 * count : 3 * count] = far[:half, :]
    left[other, 2 * count : 3 * count] = far_x[:half, :]
    left[mine, 3 * count :] = cross[half:, :]
    left[other, 3 * count :] = cross_x[half:, :]

    def body(at):
        total = jnp.dot(left[...], stacked(rights, at), preferred_element_type=jnp.float32)
        parts = [total[s * rows : (s + 1) * rows] for s in range(4)]
        mine_out[:, at] = parts[0]
        side[:rows, at] = parts[1].astype(side.dtype)
        across[:, at] = parts[2].astype(across.dtype)
        if final:
            third[0][:, at] = parts[3].astype(side.dtype)
        else:
            side[rows:, at] = parts[3].astype(side.dtype)

    each_tile(rights[0].shape[1], body)


def add_kernel(across, side, out):
    rows = across.shape[0]
    out[...] = (across[...] + side[rows:, :].astype(jnp.float32)).astype(out.dtype)


def stacked(chunks, at):
    return jnp.concatenate([chunk[:, at] for chunk in chunks], axis=0)


def flipped(zs, me_ref, rep_ref):
    return ((me_ref[0] // (2 * zs)) ^ rep_ref[0]) & 1


def out_rows(turned, chunks):
    base, value = 0, None
    for piece in turned:
        at = slice(base, base + piece.shape[0])
        term = jnp.dot(stacked(chunks, at), piece[...], preferred_element_type=jnp.float32)
        value = term if value is None else value + term
        base = at.stop
    return value


def back_term(left, chunks, at):
    order = chunks[0::2] + chunks[1::2]
    return jnp.dot(left[...], stacked(order, at), preferred_element_type=jnp.float32)


def near_kernel(zs, pieces, me_ref, rep_ref, *refs):
    turned, left, chunks = refs[:pieces], refs[pieces], refs[pieces + 1 : pieces + 1 + 2 * zs]
    keep, send, early, total = refs[pieces + 1 + 2 * zs :]
    total[...] = out_rows(turned, chunks)
    half = keep.shape[0]
    flip = flipped(zs, me_ref, rep_ref)
    keep[...] = total[pl.ds(pl.multiple_of(flip * half, half), half), :]
    send[...] = total[pl.ds(pl.multiple_of((1 - flip) * half, half), half), :]

    def body(at):
        early[:, at] = back_term(left, chunks, at)

    each_tile(early.shape[1], body)


def middle_kernel(zs, pieces, me_ref, rep_ref, *refs):
    turned, chunks = refs[:pieces], refs[pieces : pieces + 2 * (zs - 1)]
    keep, send, hold = refs[pieces + 2 * (zs - 1) :]
    value = out_rows(turned, chunks)
    span = keep.shape[0]
    flip = flipped(zs, me_ref, rep_ref)
    hold[...] = value[span : 2 * span]

    @pl.when(flip == 0)
    def _():
        keep[...] = value[:span]
        send[...] = value[2 * span :]

    @pl.when(flip == 1)
    def _():
        keep[...] = value[2 * span :]
        send[...] = value[:span]


def last_kernel(zs, pieces, me_ref, rep_ref, *refs):
    turned, (hold, one, two, keep, send) = refs[:pieces], refs[pieces:]
    value = out_rows(turned, (one, two))
    flip = flipped(zs, me_ref, rep_ref)

    @pl.when(flip == 0)
    def _():
        keep[...] = hold[...]
        send[...] = value

    @pl.when(flip == 1)
    def _():
        keep[...] = value
        send[...] = hold[...]


def store_tile(index, at, sems, pairs):
    copies = []
    for k, (source, target) in enumerate(pairs):
        copy = pltpu.make_async_copy(
            source.at[:, at], target.at[:, at], sems.at[index * len(pairs) + k]
        )
        copy.start()
        copies.append(copy)
    return copies


def slopes_kernel(gate_ref, up_ref, gate_slope, up_slope):
    def body(at):
        gate = gate_ref[:, at].astype(jnp.float32)
        sig = jax.nn.sigmoid(gate)
        gate_slope[:, at] = up_ref[:, at].astype(jnp.float32) * sig * (1.0 + gate * (1.0 - sig))
        up_slope[:, at] = gate * sig

    each_tile(gate_ref.shape[1], body)


def back_kernel(zs, left, gate_slope, up_slope, early, *refs):
    chunks, (gate_out, up_out, gate_tiles, up_tiles, sems) = refs[: 2 * zs], refs[2 * zs :]
    copies = []

    def body(at):
        hid_grad = early[:, at] + back_term(left, chunks, at)
        gate_tiles[:, at] = (hid_grad * gate_slope[:, at]).astype(jnp.bfloat16)
        up_tiles[:, at] = (hid_grad * up_slope[:, at]).astype(jnp.bfloat16)
        pairs = ((gate_tiles, gate_out), (up_tiles, up_out))
        copies.extend(store_tile(len(copies) // 2, at, sems, pairs))

    each_tile(gate_out.shape[1], body)
    for copy in copies:
        copy.wait()


def merge_kernel(zs, rows, me_ref, *refs):
    keep, got, middle, got_middle, last, got_last, out, placed = refs
    me = me_ref[0]

    def place(value, first, far):
        for s in range(value.shape[0] // (2 * rows)):
            for core in range(2):
                block = me ^ (4 * (first + s) + 2 * far + core)
                start = pl.multiple_of((block % (2 * zs)) * rows, rows)
                at = (2 * s + core) * rows
                placed[pl.ds(start, rows), :] = value[at : at + rows, :].astype(placed.dtype)

    place(keep[...] + got[...], 0, 0)
    place(middle[...] + got_middle[...], 0, 1)
    place(last[...] + got_last[...], 1, 1)
    out[...] = placed[...].T


def adamw_kernel(total, counts, *refs):
    given = sum(counts)
    parts, states = refs[:given], refs[given : given + 3]
    outs, values, sems = refs[given + 3 : given + 6], refs[given + 6 : -1], refs[-1]
    rows = outs[0].shape[0]
    base, copies = 0, []
    for p, count in enumerate(counts):
        first = sum(counts[:p])
        own, *others = parts[first : first + count]
        at = slice(base, base + own.shape[1])
        base = at.stop
        grad = own[...]
        for other in others:
            grad = grad + other[:rows, :].astype(jnp.float32)
        results = adamw(grad * jnp.float32(1.0 / total), *[state[:, at] for state in states])
        for tile, value in zip(values, results):
            tile[:, at] = value
        copies.extend(store_tile(p, at, sems, tuple(zip(values, outs))))
    for copy in copies:
        copy.wait()


def estimate(flops, moved):
    return pl.CostEstimate(flops=int(flops), bytes_accessed=int(moved), transcendentals=0)


def call(kernel, outs, ins, scratch=(), smem=0, flops=0, copied=False):
    moved = sum(v.size * v.dtype.itemsize for v in list(ins) + list(outs))
    return pl.pallas_call(
        kernel,
        out_shape=list(outs),
        in_specs=[SMEM] * smem + [VMEM] * (len(ins) - smem),
        out_specs=[pl.BlockSpec(memory_space=pl.ANY) if copied else VMEM] * len(outs),
        scratch_shapes=list(scratch),
        compiler_params=pltpu.CompilerParams(vmem_limit_bytes=24 << 20),
        cost_estimate=estimate(flops, moved),
    )(*ins)


def direct(gate_pre, up_pre, out_grad, master, moment_one, moment_two):
    n = lax.axis_size("dp")
    zs = n // 4
    micro, span, width = gate_pre.shape
    tokens = micro * span
    depth = out_grad.shape[2]
    rows = master.shape[0]
    total = micro * span * n
    me_arr = jnp.full((1,), lax.axis_index("dp"), jnp.int32)
    rep_arr = jnp.full((1,), lax.axis_index("rep"), jnp.int32)
    tiles = width // TILE
    pieces = len(SHARES)
    cuts = [tiles * sum(SHARES[:p]) // sum(SHARES) * TILE for p in range(pieces + 1)]

    def swap(value, m):
        return lax.ppermute(value, "dp", [(i, i ^ m) for i in range(n)])

    def bf16(*shape):
        return jax.ShapeDtypeStruct(shape, jnp.bfloat16)

    def f32(*shape):
        return jax.ShapeDtypeStruct(shape, jnp.float32)

    gate = gate_pre.reshape(tokens, width)
    up_val = up_pre.reshape(tokens, width)
    cotangent = out_grad.reshape(tokens, depth)

    chunk = {0: lax.optimization_barrier(master.astype(jnp.bfloat16))}
    chunk[2] = swap(chunk[0], 2)
    chunk[4] = swap(chunk[0], 4)
    chunk[8] = swap(chunk[0], 8)
    chunk[12] = swap(chunk[8], 4)
    chunk[6] = swap(chunk[2], 4)
    chunk[10] = swap(chunk[8], 2)
    chunk[14] = swap(chunk[12], 2)
    for s in range(zs):
        chunk[4 * s + 1] = swap(chunk[4 * s], 1)
        chunk[4 * s + 3] = swap(chunk[4 * s + 2], 1)

    def across_rep(value):
        return lax.ppermute(value, "rep", [(0, 1), (1, 0)])

    picked = call(
        functools.partial(select_kernel, zs, rows),
        [bf16(zs * rows, tokens)] * 3 + [bf16(2 * zs * rows, tokens)],
        [me_arr, rep_arr, cotangent],
        [pltpu.VMEM((depth, tokens), jnp.bfloat16)],
        smem=2,
    )
    far_half = swap(picked[2], 2)
    far_rest = across_rep(far_half)
    lefts = [
        picked[0], swap(picked[1], 1), far_half, far_rest, swap(far_half, 1), swap(far_rest, 1)
    ]
    hidden, sums = [], []
    for p, (lo, hi) in enumerate(zip(cuts[:-1], cuts[1:])):
        own = gated(gate[:, lo:hi], up_val[:, lo:hi])
        hidden.append(own)
        across = swap(own, 2)
        rights = [own, swap(own, 1), across, swap(across, 1)]
        size = hi - lo
        final = p == pieces - 1
        own_sum, side, across, *third = call(
            functools.partial(grads_kernel, rows, final),
            [f32(rows, size)]
            + ([bf16(rows, size)] * 3 if final else [bf16(2 * rows, size), f32(rows, size)]),
            [rep_arr] + lefts + rights,
            [pltpu.VMEM((zs * rows, 4 * tokens), jnp.bfloat16)],
            smem=1,
            flops=8 * zs * rows * tokens * size,
        )
        side = swap(side, 4)
        if not final:
            (across,) = call(add_kernel, [bf16(rows, size)], [across, side])
        across = swap(across, 8)
        sums.append([own_sum, side, across, *[swap(value, 12) for value in third]])
    *turned, left_near, left_far = call(
        functools.partial(turn_kernel, pieces),
        [bf16(h.shape[1], tokens) for h in hidden] + [bf16(tokens, depth // 2)] * 2,
        hidden + [picked[0], picked[1], picked[3]],
    )

    near = [chunk[4 * s + m] for s in range(zs) for m in (0, 1)]
    far = [chunk[4 * s + m] for s in range(zs) for m in (2, 3)]
    deep, half = depth // 2, depth // 4
    last = 2 * rows
    work = 2 * tokens * deep * width
    keep, send, early = call(
        functools.partial(near_kernel, zs, pieces),
        [f32(half, tokens), f32(half, tokens), f32(tokens, width)],
        [me_arr, rep_arr, *turned, left_near, *near],
        [pltpu.VMEM((deep, tokens), jnp.float32)],
        smem=2,
        flops=2 * work,
    )
    got = across_rep(send)
    middle, send_middle, hold = call(
        functools.partial(middle_kernel, zs, pieces),
        [f32(last, tokens)] * 3,
        [me_arr, rep_arr, *turned, *far[:-2]],
        smem=2,
        flops=work,
    )
    got_middle = across_rep(send_middle)
    keep_last, send_last = call(
        functools.partial(last_kernel, zs, pieces),
        [f32(last, tokens)] * 2,
        [me_arr, rep_arr, *turned, hold, *far[-2:]],
        smem=2,
        flops=work // zs,
    )
    got_last = across_rep(send_last)
    slopes = call(slopes_kernel, [f32(tokens, width)] * 2, [gate, up_val])
    gate_grad, up_grad = call(
        functools.partial(back_kernel, zs),
        [bf16(tokens, width)] * 2,
        [left_far, *slopes, early, *far],
        [pltpu.VMEM((tokens, width), jnp.bfloat16)] * 2 + [pltpu.SemaphoreType.DMA((2 * tiles,))],
        flops=work,
        copied=True,
    )
    (out,) = call(
        functools.partial(merge_kernel, zs, rows),
        [bf16(tokens, 2 * half)],
        [me_arr, keep, got, middle, got_middle, keep_last, got_last],
        [pltpu.VMEM((2 * half, tokens), jnp.bfloat16)],
        smem=1,
    )
    master_new, first, second = call(
        functools.partial(adamw_kernel, total, [len(parts) for parts in sums]),
        [f32(rows, width)] * 3,
        [v for parts in sums for v in parts] + [master, moment_one, moment_two],
        [pltpu.VMEM((rows, width), jnp.float32)] * 3 + [pltpu.SemaphoreType.DMA((3 * pieces,))],
        copied=True,
    )
    return (
        out.reshape(micro, span, 2 * half),
        gate_grad.reshape(gate_pre.shape),
        up_grad.reshape(gate_pre.shape),
        master_new,
        first,
        second,
    )


SHARES = (4, 4, 3)


def small(n, reps, width):
    return n == 16 and reps == 2 and width % TILE == 0


def on_device(gate_pre, *rest):
    if small(lax.axis_size("dp"), lax.axis_size("rep"), gate_pre.shape[2]):
        return direct(gate_pre, *rest)
    return plain(gate_pre, *rest)


def solution(mesh):
    placed = (
        P(None, "dp", "rep"),
        P(None, "dp", "rep"),
        P(None, "dp", None),
        P("dp", "rep"),
        P("dp", "rep"),
        P("dp", "rep"),
    )
    return jax.shard_map(
        on_device,
        mesh=mesh,
        in_specs=placed,
        out_specs=(
            P(None, "dp", "rep"),
            P(None, "dp", "rep"),
            P(None, "dp", "rep"),
            P("dp", "rep"),
            P("dp", "rep"),
            P("dp", "rep"),
        ),
        check_vma=False,
    )
```

```python
import functools
import jax
import jax.numpy as jnp
from jax import lax
from jax.experimental import pallas as pl
from jax.experimental.pallas import tpu as pltpu
from jax.sharding import PartitionSpec as P


first_power = 2.6561398887587544e-05
second_power = 0.005920529220333997


VMEM = pl.BlockSpec(memory_space=pltpu.VMEM)
SMEM = pl.BlockSpec(memory_space=pltpu.SMEM)
TILE = 256


def adamw(main_grad, master, moment_one, moment_two):
    first = 0.9 * moment_one + 0.1 * main_grad
    second = 0.95 * moment_two + 0.05 * main_grad * main_grad
    scaled = first * (1.0 / (1.0 - first_power))
    update = scaled / (jnp.sqrt(second * (1.0 / (1.0 - second_power))) + 1e-08)
    return master - 0.003 * (update + 0.1 * master), first, second


def gated(gate, up_val):
    gate = gate.astype(jnp.float32)
    return (gate * jax.nn.sigmoid(gate) * up_val.astype(jnp.float32)).astype(jnp.bfloat16)


def plain(gate_pre, up_pre, out_grad, master, moment_one, moment_two):
    micro, rows, width = gate_pre.shape
    total = micro * rows * lax.axis_size("dp")
    weights = lax.all_gather(master.astype(jnp.bfloat16), "dp", axis=0, tiled=True)
    hidden = gated(gate_pre, up_pre).reshape(-1, width)
    cotangent = out_grad.reshape(-1, out_grad.shape[2])
    grads = lax.dot_general(
        cotangent, hidden, (((0,), (0,)), ((), ())), preferred_element_type=jnp.float32
    )
    part = lax.dot_general(
        hidden, weights, (((1,), (1,)), ((), ())), preferred_element_type=jnp.float32
    )
    hid_grad = jnp.dot(cotangent, weights, preferred_element_type=jnp.float32)
    grads = lax.psum_scatter(grads, "dp", scatter_dimension=0, tiled=True)
    out = lax.psum_scatter(part, "rep", scatter_dimension=1, tiled=True).astype(jnp.bfloat16)
    gate = gate_pre.reshape(-1, width).astype(jnp.float32)
    up_val = up_pre.reshape(-1, width).astype(jnp.float32)
    sig = jax.nn.sigmoid(gate)
    gate_grad = (hid_grad * up_val * sig * (1.0 + gate * (1.0 - sig))).astype(jnp.bfloat16)
    up_grad = (hid_grad * gate * sig).astype(jnp.bfloat16)
    master_new, first, second = adamw(
        grads / jnp.float32(total), master, moment_one, moment_two
    )
    return (
        out.reshape(micro, rows, -1),
        gate_grad.reshape(gate_pre.shape),
        up_grad.reshape(gate_pre.shape),
        master_new,
        first,
        second,
    )


def select_kernel(zs, rows, me_ref, rep_ref, og_ref, own, near, far, rest, turned):
    turned[...] = og_ref[...].T
    me, rep = me_ref[0], rep_ref[0]

    def block(s, m):
        start = pl.multiple_of((me ^ (4 * s) ^ m) * rows, rows)
        return turned[pl.ds(start, rows), :]

    for s in range(zs):
        own[s * rows : (s + 1) * rows, :] = block(s, 0)
        near[s * rows : (s + 1) * rows, :] = block(s, 1)
    for m in (2, 3):
        for i in range(zs // 2):
            first = ((m - 2) * (zs // 2) + i) * rows
            far[first : first + rows, :] = block(rep * (zs // 2) + i, m)
        for s in range(zs):
            first = ((m - 2) * zs + s) * rows
            rest[first : first + rows, :] = block(s, m)


def turn_kernel(count, *refs):
    hidden, (own, near, rest) = refs[:count], refs[count : count + 3]
    turned, (left_near, left_far) = refs[count + 3 : 2 * count + 3], refs[2 * count + 3 :]
    for source, target in zip(hidden, turned):
        target[...] = source[...].T
    width = own.shape[0]
    left_near[:, :width] = own[...].T
    left_near[:, width:] = near[...].T
    left_far[...] = rest[...].T


def each_tile(width, body):
    for start in range(0, width, TILE):
        body(slice(start, start + TILE))


def grads_kernel(rows, final, rep_ref, *refs):
    own, near, far, far_x, cross, cross_x = refs[:6]
    rights, (mine_out, side, across, *third), left = refs[6:10], refs[10:-1], refs[-1]
    count = own.shape[1]
    half = 2 * rows
    mine = pl.ds(pl.multiple_of(rep_ref[0] * half, half), half)
    other = pl.ds(pl.multiple_of((1 - rep_ref[0]) * half, half), half)
    left[:, :count] = own[...]
    left[:, count : 2 * count] = near[...]
    left[mine, 2 * count : 3 * count] = far[:half, :]
    left[other, 2 * count : 3 * count] = far_x[:half, :]
    left[mine, 3 * count :] = cross[half:, :]
    left[other, 3 * count :] = cross_x[half:, :]

    def body(at):
        total = jnp.dot(left[...], stacked(rights, at), preferred_element_type=jnp.float32)
        parts = [total[s * rows : (s + 1) * rows] for s in range(4)]
        mine_out[:, at] = parts[0]
        side[:rows, at] = parts[1].astype(side.dtype)
        across[:, at] = parts[2].astype(across.dtype)
        if final:
            third[0][:, at] = parts[3].astype(side.dtype)
        else:
            side[rows:, at] = parts[3].astype(side.dtype)

    each_tile(rights[0].shape[1], body)


def add_kernel(across, side, out):
    rows = across.shape[0]
    out[...] = (across[...] + side[rows:, :].astype(jnp.float32)).astype(out.dtype)


def stacked(chunks, at):
    return jnp.concatenate([chunk[:, at] for chunk in chunks], axis=0)


def flipped(zs, me_ref, rep_ref):
    return ((me_ref[0] // (2 * zs)) ^ rep_ref[0]) & 1


def out_rows(turned, chunks):
    base, value = 0, None
    for piece in turned:
        at = slice(base, base + piece.shape[0])
        term = jnp.dot(stacked(chunks, at), piece[...], preferred_element_type=jnp.float32)
        value = term if value is None else value + term
        base = at.stop
    return value


def back_term(left, chunks, at):
    order = chunks[0::2] + chunks[1::2]
    return jnp.dot(left[...], stacked(order, at), preferred_element_type=jnp.float32)


def near_kernel(zs, pieces, me_ref, rep_ref, *refs):
    turned, left, chunks = refs[:pieces], refs[pieces], refs[pieces + 1 : pieces + 1 + 2 * zs]
    keep, send, early, total = refs[pieces + 1 + 2 * zs :]
    total[...] = out_rows(turned, chunks)
    half = keep.shape[0]
    flip = flipped(zs, me_ref, rep_ref)
    keep[...] = total[pl.ds(pl.multiple_of(flip * half, half), half), :]
    send[...] = total[pl.ds(pl.multiple_of((1 - flip) * half, half), half), :]

    def body(at):
        early[:, at] = back_term(left, chunks, at)

    each_tile(early.shape[1], body)


def middle_kernel(zs, pieces, me_ref, rep_ref, *refs):
    turned, chunks = refs[:pieces], refs[pieces : pieces + 2 * (zs - 1)]
    keep, send, hold = refs[pieces + 2 * (zs - 1) :]
    value = out_rows(turned, chunks)
    span = keep.shape[0]
    flip = flipped(zs, me_ref, rep_ref)
    hold[...] = value[span : 2 * span]

    @pl.when(flip == 0)
    def _():
        keep[...] = value[:span]
        send[...] = value[2 * span :]

    @pl.when(flip == 1)
    def _():
        keep[...] = value[2 * span :]
        send[...] = value[:span]


def last_kernel(zs, pieces, me_ref, rep_ref, *refs):
    turned, (hold, first, one, two, keep, send) = refs[:pieces], refs[pieces:]
    value = out_rows(turned, (one, two))
    flip = flipped(zs, me_ref, rep_ref)
    span = keep.shape[0]
    send[:span, :] = first[...].astype(send.dtype)

    @pl.when(flip == 0)
    def _():
        keep[...] = hold[...]
        send[span:, :] = value.astype(send.dtype)

    @pl.when(flip == 1)
    def _():
        keep[...] = value
        send[span:, :] = hold[...].astype(send.dtype)


def store_tile(index, at, sems, pairs):
    copies = []
    for k, (source, target) in enumerate(pairs):
        copy = pltpu.make_async_copy(
            source.at[:, at], target.at[:, at], sems.at[index * len(pairs) + k]
        )
        copy.start()
        copies.append(copy)
    return copies


def slopes_kernel(gate_ref, up_ref, gate_slope, up_slope):
    def body(at):
        gate = gate_ref[:, at].astype(jnp.float32)
        sig = jax.nn.sigmoid(gate)
        gate_slope[:, at] = up_ref[:, at].astype(jnp.float32) * sig * (1.0 + gate * (1.0 - sig))
        up_slope[:, at] = gate * sig

    each_tile(gate_ref.shape[1], body)


def back_kernel(zs, left, gate_slope, up_slope, early, *refs):
    chunks, (gate_out, up_out, gate_tiles, up_tiles, sems) = refs[: 2 * zs], refs[2 * zs :]
    copies = []

    def body(at):
        hid_grad = early[:, at] + back_term(left, chunks, at)
        gate_tiles[:, at] = (hid_grad * gate_slope[:, at]).astype(jnp.bfloat16)
        up_tiles[:, at] = (hid_grad * up_slope[:, at]).astype(jnp.bfloat16)
        pairs = ((gate_tiles, gate_out), (up_tiles, up_out))
        copies.extend(store_tile(len(copies) // 2, at, sems, pairs))

    each_tile(gate_out.shape[1], body)
    for copy in copies:
        copy.wait()


def merge_kernel(zs, rows, me_ref, *refs):
    keep, got, middle, last, got_far, out, placed = refs
    span = last.shape[0]
    me = me_ref[0]

    def place(value, first, far):
        for s in range(value.shape[0] // (2 * rows)):
            for core in range(2):
                block = me ^ (4 * (first + s) + 2 * far + core)
                start = pl.multiple_of((block % (2 * zs)) * rows, rows)
                at = (2 * s + core) * rows
                placed[pl.ds(start, rows), :] = value[at : at + rows, :].astype(placed.dtype)

    place(keep[...] + got[...], 0, 0)
    place(middle[...] + got_far[:span, :].astype(jnp.float32), 0, 1)
    place(last[...] + got_far[span:, :].astype(jnp.float32), 1, 1)
    out[...] = placed[...].T


def adamw_kernel(total, counts, *refs):
    given = sum(counts)
    parts, states = refs[:given], refs[given : given + 3]
    outs, values, sems = refs[given + 3 : given + 6], refs[given + 6 : -1], refs[-1]
    rows = outs[0].shape[0]
    base, copies = 0, []
    for p, count in enumerate(counts):
        first = sum(counts[:p])
        own, *others = parts[first : first + count]
        at = slice(base, base + own.shape[1])
        base = at.stop
        grad = own[...]
        for other in others:
            grad = grad + other[:rows, :].astype(jnp.float32)
        results = adamw(grad * jnp.float32(1.0 / total), *[state[:, at] for state in states])
        for tile, value in zip(values, results):
            tile[:, at] = value
        copies.extend(store_tile(p, at, sems, tuple(zip(values, outs))))
    for copy in copies:
        copy.wait()


def estimate(flops, moved):
    return pl.CostEstimate(flops=int(flops), bytes_accessed=int(moved), transcendentals=0)


def call(kernel, outs, ins, scratch=(), smem=0, flops=0, copied=False):
    moved = sum(v.size * v.dtype.itemsize for v in list(ins) + list(outs))
    return pl.pallas_call(
        kernel,
        out_shape=list(outs),
        in_specs=[SMEM] * smem + [VMEM] * (len(ins) - smem),
        out_specs=[pl.BlockSpec(memory_space=pl.ANY) if copied else VMEM] * len(outs),
        scratch_shapes=list(scratch),
        compiler_params=pltpu.CompilerParams(vmem_limit_bytes=24 << 20),
        cost_estimate=estimate(flops, moved),
    )(*ins)


def direct(gate_pre, up_pre, out_grad, master, moment_one, moment_two):
    n = lax.axis_size("dp")
    zs = n // 4
    micro, span, width = gate_pre.shape
    tokens = micro * span
    depth = out_grad.shape[2]
    rows = master.shape[0]
    total = micro * span * n
    me_arr = jnp.full((1,), lax.axis_index("dp"), jnp.int32)
    rep_arr = jnp.full((1,), lax.axis_index("rep"), jnp.int32)
    tiles = width // TILE
    pieces = len(SHARES)
    cuts = [tiles * sum(SHARES[:p]) // sum(SHARES) * TILE for p in range(pieces + 1)]

    def swap(value, m):
        return lax.ppermute(value, "dp", [(i, i ^ m) for i in range(n)])

    def bf16(*shape):
        return jax.ShapeDtypeStruct(shape, jnp.bfloat16)

    def f32(*shape):
        return jax.ShapeDtypeStruct(shape, jnp.float32)

    gate = gate_pre.reshape(tokens, width)
    up_val = up_pre.reshape(tokens, width)
    cotangent = out_grad.reshape(tokens, depth)

    chunk = {0: lax.optimization_barrier(master.astype(jnp.bfloat16))}
    chunk[2] = swap(chunk[0], 2)
    chunk[4] = swap(chunk[0], 4)
    chunk[8] = swap(chunk[0], 8)
    chunk[12] = swap(chunk[8], 4)
    chunk[6] = swap(chunk[2], 4)
    chunk[10] = swap(chunk[8], 2)
    chunk[14] = swap(chunk[12], 2)
    for s in range(zs):
        chunk[4 * s + 1] = swap(chunk[4 * s], 1)
        chunk[4 * s + 3] = swap(chunk[4 * s + 2], 1)

    def across_rep(value):
        return lax.ppermute(value, "rep", [(0, 1), (1, 0)])

    picked = call(
        functools.partial(select_kernel, zs, rows),
        [bf16(zs * rows, tokens)] * 3 + [bf16(2 * zs * rows, tokens)],
        [me_arr, rep_arr, cotangent],
        [pltpu.VMEM((depth, tokens), jnp.bfloat16)],
        smem=2,
    )
    far_half = swap(picked[2], 2)
    far_rest = across_rep(far_half)
    lefts = [
        picked[0], swap(picked[1], 1), far_half, far_rest, swap(far_half, 1), swap(far_rest, 1)
    ]
    hidden, sums = [], []
    for p, (lo, hi) in enumerate(zip(cuts[:-1], cuts[1:])):
        own = gated(gate[:, lo:hi], up_val[:, lo:hi])
        hidden.append(own)
        across = swap(own, 2)
        rights = [own, swap(own, 1), across, swap(across, 1)]
        size = hi - lo
        final = p == pieces - 1
        own_sum, side, across, *third = call(
            functools.partial(grads_kernel, rows, final),
            [f32(rows, size)]
            + ([bf16(rows, size)] * 3 if final else [bf16(2 * rows, size), f32(rows, size)]),
            [rep_arr] + lefts + rights,
            [pltpu.VMEM((zs * rows, 4 * tokens), jnp.bfloat16)],
            smem=1,
            flops=8 * zs * rows * tokens * size,
        )
        side = swap(side, 4)
        if not final:
            (across,) = call(add_kernel, [bf16(rows, size)], [across, side])
        across = swap(across, 8)
        sums.append([own_sum, side, across, *[swap(value, 12) for value in third]])
    *turned, left_near, left_far = call(
        functools.partial(turn_kernel, pieces),
        [bf16(h.shape[1], tokens) for h in hidden] + [bf16(tokens, depth // 2)] * 2,
        hidden + [picked[0], picked[1], picked[3]],
    )

    near = [chunk[4 * s + m] for s in range(zs) for m in (0, 1)]
    far = [chunk[4 * s + m] for s in range(zs) for m in (2, 3)]
    deep, half = depth // 2, depth // 4
    last = 2 * rows
    work = 2 * tokens * deep * width
    keep, send, early = call(
        functools.partial(near_kernel, zs, pieces),
        [f32(half, tokens), f32(half, tokens), f32(tokens, width)],
        [me_arr, rep_arr, *turned, left_near, *near],
        [pltpu.VMEM((deep, tokens), jnp.float32)],
        smem=2,
        flops=2 * work,
    )
    got = across_rep(send)
    middle, send_middle, hold = call(
        functools.partial(middle_kernel, zs, pieces),
        [f32(last, tokens)] * 3,
        [me_arr, rep_arr, *turned, *far[:-2]],
        smem=2,
        flops=work,
    )
    keep_last, send_last = call(
        functools.partial(last_kernel, zs, pieces),
        [f32(last, tokens), bf16(2 * last, tokens)],
        [me_arr, rep_arr, *turned, hold, send_middle, *far[-2:]],
        smem=2,
        flops=work // zs,
    )
    got_far = across_rep(send_last)
    slopes = call(slopes_kernel, [f32(tokens, width)] * 2, [gate, up_val])
    gate_grad, up_grad = call(
        functools.partial(back_kernel, zs),
        [bf16(tokens, width)] * 2,
        [left_far, *slopes, early, *far],
        [pltpu.VMEM((tokens, width), jnp.bfloat16)] * 2 + [pltpu.SemaphoreType.DMA((2 * tiles,))],
        flops=work,
        copied=True,
    )
    (out,) = call(
        functools.partial(merge_kernel, zs, rows),
        [bf16(tokens, 2 * half)],
        [me_arr, keep, got, middle, keep_last, got_far],
        [pltpu.VMEM((2 * half, tokens), jnp.bfloat16)],
        smem=1,
    )
    master_new, first, second = call(
        functools.partial(adamw_kernel, total, [len(parts) for parts in sums]),
        [f32(rows, width)] * 3,
        [v for parts in sums for v in parts] + [master, moment_one, moment_two],
        [pltpu.VMEM((rows, width), jnp.float32)] * 3 + [pltpu.SemaphoreType.DMA((3 * pieces,))],
        copied=True,
    )
    return (
        out.reshape(micro, span, 2 * half),
        gate_grad.reshape(gate_pre.shape),
        up_grad.reshape(gate_pre.shape),
        master_new,
        first,
        second,
    )


SHARES = (4, 4, 3)


def small(n, reps, width):
    return n == 16 and reps == 2 and width % TILE == 0


def on_device(gate_pre, *rest):
    if small(lax.axis_size("dp"), lax.axis_size("rep"), gate_pre.shape[2]):
        return direct(gate_pre, *rest)
    return plain(gate_pre, *rest)


def solution(mesh):
    placed = (
        P(None, "dp", "rep"),
        P(None, "dp", "rep"),
        P(None, "dp", None),
        P("dp", "rep"),
        P("dp", "rep"),
        P("dp", "rep"),
    )
    return jax.shard_map(
        on_device,
        mesh=mesh,
        in_specs=placed,
        out_specs=(
            P(None, "dp", "rep"),
            P(None, "dp", "rep"),
            P(None, "dp", "rep"),
            P("dp", "rep"),
            P("dp", "rep"),
            P("dp", "rep"),
        ),
        check_vma=False,
    )
```
